32 devices in a mesh: seq: 8 (over z, core), ch: 4 (over y, x).
Axes of the slice: x: 2, y: 2, z: 4, core: 2. Of those that a mesh axis runs over, the one named last changes fastest.
Arguments:
- input_q: bfloat16 [4096, 8192], P('seq', 'ch'), may hold values from -6 to 6
- input_k: bfloat16 [4096, 8192], P('seq', 'ch'), may hold values from -6 to 6
- input_v: bfloat16 [4096, 8192], P('seq', 'ch'), may hold values from -6 to 6
- grad_out: bfloat16 [4096, 8192], P('seq', 'ch'), may hold values from -6 to 6
- short_filters: float32 [3, 3, 8192], P(None, None, 'ch'), may hold values from -3.5 to 3.5
- long_filter: float32 [128, 8192], P(None, 'ch'), may hold values from -0.5 to 0.5
- skip_gain: float32 [8192], P('ch'), may hold values from 0.5 to 1.5
Outputs:
- grad_input_q: bfloat16 [4096, 8192], P('seq', 'ch')
- grad_input_k: bfloat16 [4096, 8192], P('seq', 'ch')
- grad_input_v: bfloat16 [4096, 8192], P('seq', 'ch')
- grad_long: float32 [128, 8192], P('seq', 'ch')
- grad_short: float32 [3, 3, 8192], P(None, None, 'ch')
- grad_skip: float32 [8192], P('ch')
The draws below stay inside these ranges and needn't reach their ends.
All inputs are finite; a program needn't handle non-finite values.
Results may differ from the reference program's by a relative error of at most 0.001.
Values may be sent and summed in bfloat16 or wider, within the bound.
No kernel may reach another device: no remote copies, remote signals or barrier semaphores. Data moves between devices by JAX's collectives and lax.ppermute only.
A program may use at most 128 MiB of HBM per device.

```python
import math
import jax
import jax.numpy as jnp
from jax import lax

D = 8192
TAPS = 3
FILT = 128
SEQ = 4096


def levels(stream_key, shape, shards, smallest, high):
    level, own = 1.0, jax.random.fold_in(stream_key, 6)
    for axis_at, shards_of in shards:
        draws = jnp.exp(jax.random.uniform(jax.random.fold_in(own, axis_at), (shards_of,), jnp.float32, smallest / len(shards), high / len(shards)))
        level = level * jnp.repeat(draws, shape[axis_at] // shards_of).reshape([-1 if axis == axis_at else 1 for axis in range(len(shape))])
    return level


def gaussian(key, dims, scale, limit, cuts=(), dtype=jnp.bfloat16):
    factor_of = levels(key, dims, cuts, -0.22, 0.18) if cuts else 1.0
    entries = jax.random.normal(key, dims, jnp.float32) * scale * factor_of
    return jnp.minimum(jnp.maximum(entries, -limit), limit).astype(dtype)


def setup_inputs(seed: int = 0) -> dict:
    arg_keys = jax.random.split(jax.random.key(seed), 8)
    return {
        "input_q": gaussian(arg_keys[0], (SEQ, D), 1.0, 6.0, ((0, 8), (1, 4))),
        "input_k": gaussian(arg_keys[1], (SEQ, D), 1.0, 6.0, ((0, 8), (1, 4))),
        "input_v": gaussian(arg_keys[2], (SEQ, D), 1.0, 6.0, ((0, 8), (1, 4))),
        "grad_out": gaussian(arg_keys[3], (SEQ, D), 1.0, 6.0, ((0, 8), (1, 4))),
        "short_filters": gaussian(arg_keys[4], (3, TAPS, D), TAPS ** -0.5, 3.5, ((2, 4),), jnp.float32),
        "long_filter": gaussian(arg_keys[5], (FILT, D), FILT ** -0.5, 0.5, ((1, 4),), jnp.float32),
        "skip_gain": jnp.clip(0.5 + 1.0 * jax.random.uniform(arg_keys[6], (D,), jnp.float32) ** levels(arg_keys[6], (D,), ((0, 4),), -0.2, 0.2), 0.5, 1.5),
    }


def one_block(packed):
    query_in, key_in, value_in, upstream, taps_w, filt, gain = packed
    length = query_in.shape[0]
    ntap = taps_w.shape[1]

    def short_conv(signal, weights):
        padded = jnp.pad(signal, ((ntap - 1, 0), (0, 0)))
        total = jnp.zeros_like(signal)
        for index in range(ntap):
            total = total + weights[index] * padded[ntap - 1 - index:ntap - 1 - index + length]
        return total

    def short_back(grad, weights, signal):
        grad_pad = jnp.pad(grad, ((0, ntap - 1), (0, 0)))
        sig_pad = jnp.pad(signal, ((ntap - 1, 0), (0, 0)))
        result = jnp.zeros_like(grad)
        rows_taps = []
        for index in range(ntap):
            result = result + weights[index] * grad_pad[index:index + length]
            rows_taps.append(jnp.sum(grad * sig_pad[ntap - 1 - index:ntap - 1 - index + length], axis=0))
        return result, jnp.stack(rows_taps)

    q_sig = query_in.astype(jnp.float32)
    k_sig = key_in.astype(jnp.float32)
    v_sig = value_in.astype(jnp.float32)
    dy_sig = upstream.astype(jnp.float32)
    q_feat = short_conv(q_sig, taps_w[0])
    k_feat = short_conv(k_sig, taps_w[1])
    v_feat = short_conv(v_sig, taps_w[2])
    z_feat = k_feat * v_feat
    double = 2 * length
    spec_h = jnp.fft.rfft(filt, n=double, axis=0)
    spec_z = jnp.fft.rfft(z_feat, n=double, axis=0)
    s_feat = jnp.fft.irfft(spec_z * spec_h, n=double, axis=0)[:length].astype(jnp.float32) + gain * z_feat
    grad_q = dy_sig * s_feat
    grad_s = dy_sig * q_feat
    spec_s = jnp.fft.rfft(grad_s, n=double, axis=0)
    grad_z = jnp.fft.irfft(spec_s * jnp.conj(spec_h), n=double, axis=0)[:length].astype(jnp.float32) + gain * grad_s
    grad_k = grad_z * v_feat
    grad_v = grad_z * k_feat
    grad_filt = jnp.fft.irfft(spec_s * jnp.conj(spec_z), n=double, axis=0)[:filt.shape[0]].astype(jnp.float32)
    grad_gain = jnp.sum(grad_s * z_feat, axis=0)
    back_q, taps_q = short_back(grad_q, taps_w[0], q_sig)
    back_k, taps_k = short_back(grad_k, taps_w[1], k_sig)
    back_v, taps_v = short_back(grad_v, taps_w[2], v_sig)
    return (back_q.astype(jnp.bfloat16), back_k.astype(jnp.bfloat16), back_v.astype(jnp.bfloat16),
            grad_filt, jnp.stack([taps_q, taps_k, taps_v]), grad_gain)


def reference(input_q, input_k, input_v, grad_out, short_filters, long_filter, skip_gain):
    length, width = input_q.shape
    block = math.gcd(width, 512)
    count = width // block

    def split(array):
        return array.reshape(array.shape[0], count, block).transpose(1, 0, 2)

    def merge(array):
        return array.transpose(1, 0, 2).reshape(array.shape[1], width)

    packed = (split(input_q), split(input_k), split(input_v), split(grad_out),
              short_filters.reshape(3, short_filters.shape[1], count, block).transpose(2, 0, 1, 3),
              split(long_filter), skip_gain.reshape(count, block))
    back_q, back_k, back_v, grad_filt, grad_taps, grad_gain = lax.map(one_block, packed)
    grad_taps = grad_taps.transpose(1, 2, 0, 3).reshape(3, short_filters.shape[1], width)
    return (merge(back_q), merge(back_k), merge(back_v), merge(grad_filt), grad_taps, grad_gain.reshape(width))
```

```python
import functools

import jax
import jax.numpy as jnp
import numpy as np
from jax import lax
from jax.experimental import pallas as pl
from jax.experimental.pallas import tpu as pltpu
from jax.sharding import PartitionSpec as P

CHUNKS = 2
LANES = 256
EDGE = 16
F32 = jnp.float32
BF16 = jnp.bfloat16


def split_np(m):
    hi = np.asarray(m, np.float32).astype(BF16)
    lo = (np.asarray(m, np.float64) - hi.astype(np.float64)).astype(np.float32).astype(BF16)
    return hi, lo


def matrices(n):
    w = 2.0 * np.pi * (np.arange(n) + 0.25) / n
    ang = np.outer(w, np.arange(n))
    fwd = np.concatenate([np.cos(ang), -np.sin(ang)], 0)
    inv = np.concatenate([np.cos(ang).T, -np.sin(ang).T], 1) / n
    fh, fl = split_np(fwd)
    ih, il = split_np(inv)
    return np.concatenate([fh, fh, fl], 1), np.concatenate([ih, ih, il], 1)


def dot3(mat, x):
    hi = x.astype(BF16)
    lo = (x - hi.astype(F32)).astype(BF16)
    return jnp.dot(mat, jnp.concatenate([hi, lo, hi], 0), preferred_element_type=F32)


def kernel(span, length, nalias, q_r, k_r, v_r, g_r, fwd_r, bwd_r, sf_r, h_r, hrev_r, fm_r, im_r, *rest):
    rest = rest[nalias:]
    oq_r, ok_r, ov_r, pl_r, ps_r = rest[:5]
    xq, xk, xv, kf, vf, zs, gs, gq, gk, gv, zsp, gsp = rest[5:]
    n = span
    nb = length // n
    halo = n + EDGE
    xq[0:EDGE] = fwd_r[2 * halo :].astype(F32)
    xq[EDGE : EDGE + length] = q_r[...].astype(F32)
    xq[EDGE + length :] = bwd_r[0:halo].astype(F32)
    xk[0:halo] = fwd_r[0:halo].astype(F32)
    xk[halo : halo + length] = k_r[...].astype(F32)
    xk[halo + length :] = bwd_r[2 * halo : 2 * halo + EDGE].astype(F32)
    xv[0:halo] = fwd_r[halo : 2 * halo].astype(F32)
    xv[halo : halo + length] = v_r[...].astype(F32)
    xv[halo + length :] = bwd_r[2 * halo + EDGE :].astype(F32)
    taps = sf_r.shape[1]
    sf = [[sf_r[a, i : i + 1, :] for i in range(taps)] for a in range(3)]
    fm = fm_r[...]
    im = im_r[...]

    def feat(ref, base, t0, rows, w):
        acc = w[0] * ref[base + t0 : base + t0 + rows]
        for i in range(1, taps):
            acc = acc + w[i] * ref[base + t0 - i : base + t0 - i + rows]
        return acc

    for b in range(-1, nb):
        t0 = b * n
        kb = feat(xk, halo, t0, n, sf[1])
        vb = feat(xv, halo, t0, n, sf[2])
        zb = kb * vb
        if b >= 0:
            kf[t0 : t0 + n] = kb
            vf[t0 : t0 + n] = vb
        zs[t0 + n : t0 + 2 * n] = zb
        zsp[b + 1] = dot3(fm, zb)
    kb = feat(xk, halo, length, 8, sf[1])
    vb = feat(xv, halo, length, 8, sf[2])
    kf[length : length + 8] = kb
    vf[length : length + 8] = vb
    zs[length + n : length + n + 8] = kb * vb
    for b in range(nb + 1):
        t0 = b * n
        qb = feat(xq, EDGE, t0, n, sf[0])
        gb = g_r[t0 : t0 + n] if b < nb else bwd_r[halo : halo + n]
        gsb = qb * gb.astype(F32)
        gs[t0 : t0 + n] = gsb
        gsp[b] = dot3(fm, gsb)
    t0 = length + n
    qb = feat(xq, EDGE, t0, 8, sf[0])
    gs[t0 : t0 + 8] = qb * bwd_r[halo + n : halo + n + EDGE].astype(F32)[0:8]

    h = h_r[...]
    hsp = dot3(fm, h)
    hr, hi = hsp[0:n], hsp[n:]
    lr = li = None
    for b in range(nb):
        t0 = b * n
        zc, zp = zsp.at[b + 1], zsp.at[b]
        gc, gn = gsp.at[b], gsp.at[b + 1]
        ur = zc[0:n] - zp[n:]
        ui = zc[n:] + zp[0:n]
        gr, gi = gc[0:n], gc[n:]
        dr = gr * ur + gi * ui
        di = gi * ur - gr * ui
        lr = dr if lr is None else lr + dr
        li = di if li is None else li + di
        s = dot3(im, jnp.concatenate([hr * ur - hi * ui, hr * ui + hi * ur], 0))
        gq[t0 : t0 + n] = s * g_r[t0 : t0 + n].astype(F32)
        wr = gr + gn[n:]
        wi = gi - gn[0:n]
        gz = dot3(im, jnp.concatenate([hr * wr + hi * wi, hr * wi - hi * wr], 0))
        gk[t0 : t0 + n] = gz * vf[t0 : t0 + n]
        gv[t0 : t0 + n] = gz * kf[t0 : t0 + n]
    long = dot3(im, jnp.concatenate([lr, li], 0))
    pl_r[...] = long

    hrev = hrev_r[...]
    g_edge = bwd_r[halo : halo + EDGE].astype(F32)
    for r in range(taps - 1):
        at = length + n - (n - 1) + r
        sr = jnp.sum(hrev * zs[at : at + n], 0, keepdims=True)
        gzr = jnp.sum(h * gs[length + r : length + r + n], 0, keepdims=True)
        gq[length + r : length + r + 1] = sr * g_edge[r : r + 1]
        gk[length + r : length + r + 1] = gzr * vf[length + r : length + r + 1]
        gv[length + r : length + r + 1] = gzr * kf[length + r : length + r + 1]

    rows = []
    for a, (grad, x, base, out) in enumerate(((gq, xq, EDGE, oq_r), (gk, xk, halo, ok_r), (gv, xv, halo, ov_r))):
        sums = [None] * taps
        for b in range(nb):
            t0 = b * n
            own = grad[t0 : t0 + n]
            acc = sf[a][0] * own
            for i in range(1, taps):
                acc = acc + sf[a][i] * grad[t0 + i : t0 + i + n]
            out[t0 : t0 + n] = acc.astype(BF16)
            for i in range(taps):
                part = jnp.sum(own * x[base + t0 - i : base + t0 - i + n], 0, keepdims=True)
                sums[i] = part if sums[i] is None else sums[i] + part
        rows += sums
    rows.append(long[0:1])
    for i, row in enumerate(rows):
        ps_r[i : i + 1] = row


def shifted(value, axis, by):
    size = lax.axis_size(axis)
    pairs = [(i, i + by) for i in range(size) if 0 <= i + by < size]
    return lax.ppermute(value, axis, pairs)


def reduce_parts(long, small, axis):
    size = lax.axis_size(axis)
    me = lax.axis_index(axis)
    if size & (size - 1):
        return lax.psum_scatter(long, axis, scatter_dimension=0, tiled=True), lax.psum(small, axis)
    piece = long.shape[0] // size
    width = long.shape[1]
    cur = long.reshape((size, piece, width))
    dist = 1
    while dist < size:
        bit = (me // dist) % 2
        pair = cur.reshape((cur.shape[0] // 2, 2, piece, width))
        keep = jnp.where(bit == 0, pair[:, 0], pair[:, 1])
        send = jnp.where(bit == 0, pair[:, 1], pair[:, 0])
        half = keep.shape[0]
        pack = jnp.concatenate([send.reshape(half * piece, width), small], 0)
        got = lax.ppermute(pack, axis, [(i, i ^ dist) for i in range(size)])
        cur = keep + got[: half * piece].reshape(half, piece, width)
        small = small + got[half * piece :]
        dist *= 2
    return cur[0], small


def body(input_q, input_k, input_v, grad_out, short_filters, long_filter, skip_gain):
    length, width = input_q.shape
    taps = short_filters.shape[1]
    n = long_filter.shape[0]
    halo = n + EDGE
    lanes = LANES
    cw = width // CHUNKS
    steps = cw // lanes
    fm, im = matrices(n)
    fm = jnp.asarray(fm)
    im = jnp.asarray(im)
    hg = long_filter.at[0].add(skip_gain)
    hrev = hg[::-1]
    arrays = (input_q, input_k, input_v, grad_out)
    outs = ()
    halos = []
    for c in range(CHUNKS):
        cs = slice(c * cw, (c + 1) * cw)
        tail = jnp.concatenate([input_k[length - halo :, cs], input_v[length - halo :, cs], input_q[length - EDGE :, cs]], 0)
        head = jnp.concatenate([input_q[:halo, cs], grad_out[:halo, cs], input_k[:EDGE, cs], input_v[:EDGE, cs]], 0)
        halos.append((shifted(tail, "seq", 1), shifted(head, "seq", -1)))
    small_rows = 3 * taps + 1
    parts = []
    for c in range(CHUNKS):
        col = lambda i, c=c: (0, c * steps + i)
        own = lambda i: (0, i)
        full = pl.BlockSpec((length, lanes), col)
        fixed = lambda a: pl.BlockSpec(a.shape, lambda i: (0, 0))
        fwd, bwd = halos[c]
        res = pl.pallas_call(
            functools.partial(kernel, n, length, len(outs)),
            grid=(steps,),
            in_specs=[full] * 4
            + [
                pl.BlockSpec((fwd.shape[0], lanes), own),
                pl.BlockSpec((bwd.shape[0], lanes), own),
                pl.BlockSpec((3, taps, lanes), lambda i, c=c: (0, 0, c * steps + i)),
                pl.BlockSpec((n, lanes), col),
                pl.BlockSpec((n, lanes), col),
                fixed(fm),
                fixed(im),
            ]
            + [pl.BlockSpec(memory_space=pl.ANY)] * len(outs),
            out_specs=[full] * 3 + [pl.BlockSpec((n, lanes), own), pl.BlockSpec((small_rows, lanes), own)],
            out_shape=[jax.ShapeDtypeStruct((length, width), BF16)] * 3
            + [jax.ShapeDtypeStruct((n, cw), F32), jax.ShapeDtypeStruct((small_rows, cw), F32)],
            scratch_shapes=[
                pltpu.VMEM((EDGE + length + halo, lanes), F32),
                pltpu.VMEM((halo + length + EDGE, lanes), F32),
                pltpu.VMEM((halo + length + EDGE, lanes), F32),
                pltpu.VMEM((length + 8, lanes), F32),
                pltpu.VMEM((length + 8, lanes), F32),
                pltpu.VMEM((n + length + 8, lanes), F32),
                pltpu.VMEM((length + n + 8, lanes), F32),
                pltpu.VMEM((length + 8, lanes), F32),
                pltpu.VMEM((length + 8, lanes), F32),
                pltpu.VMEM((length + 8, lanes), F32),
                pltpu.VMEM((length // n + 1, 2 * n, lanes), F32),
                pltpu.VMEM((length // n + 1, 2 * n, lanes), F32),
            ],
            input_output_aliases={11 + j: j for j in range(len(outs))},
            name=f"hyena_bwd_{c}",
        )(*arrays, fwd, bwd, short_filters, hg, hrev, fm, im, *outs)
        outs = tuple(res[:3])
        parts.append(reduce_parts(res[3], res[4], "seq"))
    grad_long = jnp.concatenate([p[0] for p in parts], 1)
    small = jnp.concatenate([p[1] for p in parts], 1)
    return outs + (grad_long, small[: 3 * taps].reshape(3, taps, width), small[3 * taps])


def solution(mesh):
    return jax.shard_map(
        body,
        mesh=mesh,
        in_specs=(
            P("seq", "ch"),
            P("seq", "ch"),
            P("seq", "ch"),
            P("seq", "ch"),
            P(None, None, "ch"),
            P(None, "ch"),
            P("ch"),
        ),
        out_specs=(
            P("seq", "ch"),
            P("seq", "ch"),
            P("seq", "ch"),
            P("seq", "ch"),
            P(None, None, "ch"),
            P("ch"),
        ),
        check_vma=False,
    )
```

```python
import functools

import jax
import jax.numpy as jnp
import numpy as np
from jax import lax
from jax.experimental import pallas as pl
from jax.experimental.pallas import tpu as pltpu
from jax.sharding import PartitionSpec as P

CHUNKS = 2
LANES = 256
EDGE = 16
F32 = jnp.float32
BF16 = jnp.bfloat16


def split_np(m):
    hi = np.asarray(m, np.float32).astype(BF16)
    lo = (np.asarray(m, np.float64) - hi.astype(np.float64)).astype(np.float32).astype(BF16)
    return hi, lo


def matrices(n):
    w = 2.0 * np.pi * (np.arange(n) + 0.25) / n
    ang = np.outer(w, np.arange(n))
    fwd = np.concatenate([np.cos(ang), -np.sin(ang)], 0)
    inv = np.concatenate([np.cos(ang).T, -np.sin(ang).T], 1) / n
    fh, fl = split_np(fwd)
    ih, il = split_np(inv)
    return np.concatenate([fh, fh, fl], 1), np.concatenate([ih, ih, il], 1)


def dot3(mat, x):
    hi = x.astype(BF16)
    lo = (x - hi.astype(F32)).astype(BF16)
    return jnp.dot(mat, jnp.concatenate([hi, lo, hi], 0), preferred_element_type=F32)


def kernel(span, length, nalias, q_r, k_r, v_r, g_r, fwd_r, bwd_r, sf_r, h_r, gain_r, fm_r, im_r, rev_r, *rest):
    rest = rest[nalias:]
    oq_r, ok_r, ov_r, pl_r, ps_r = rest[:5]
    xq, xk, xv, kf, vf, zs, gs, gq, gk, gv, zsp, gsp = rest[5:]
    n = span
    nb = length // n
    halo = n + EDGE
    xq[0:EDGE] = fwd_r[2 * halo :].astype(F32)
    xq[EDGE : EDGE + length] = q_r[...].astype(F32)
    xq[EDGE + length :] = bwd_r[0:halo].astype(F32)
    xk[0:halo] = fwd_r[0:halo].astype(F32)
    xk[halo : halo + length] = k_r[...].astype(F32)
    xk[halo + length :] = bwd_r[2 * halo : 2 * halo + EDGE].astype(F32)
    xv[0:halo] = fwd_r[halo : 2 * halo].astype(F32)
    xv[halo : halo + length] = v_r[...].astype(F32)
    xv[halo + length :] = bwd_r[2 * halo + EDGE :].astype(F32)
    taps = sf_r.shape[1]
    sf = [[sf_r[a, i : i + 1, :] for i in range(taps)] for a in range(3)]
    fm = fm_r[...]
    im = im_r[...]

    def feat(ref, base, t0, rows, w):
        acc = w[0] * ref[base + t0 : base + t0 + rows]
        for i in range(1, taps):
            acc = acc + w[i] * ref[base + t0 - i : base + t0 - i + rows]
        return acc

    for b in range(-1, nb):
        t0 = b * n
        kb = feat(xk, halo, t0, n, sf[1])
        vb = feat(xv, halo, t0, n, sf[2])
        zb = kb * vb
        if b >= 0:
            kf[t0 : t0 + n] = kb
            vf[t0 : t0 + n] = vb
        zs[t0 + n : t0 + 2 * n] = zb
        zsp[b + 1] = dot3(fm, zb)
    kb = feat(xk, halo, length, 8, sf[1])
    vb = feat(xv, halo, length, 8, sf[2])
    kf[length : length + 8] = kb
    vf[length : length + 8] = vb
    zs[length + n : length + n + 8] = kb * vb
    for b in range(nb + 1):
        t0 = b * n
        qb = feat(xq, EDGE, t0, n, sf[0])
        gb = g_r[t0 : t0 + n] if b < nb else bwd_r[halo : halo + n]
        gsb = qb * gb.astype(F32)
        gs[t0 : t0 + n] = gsb
        gsp[b] = dot3(fm, gsb)
    t0 = length + n
    qb = feat(xq, EDGE, t0, 8, sf[0])
    gs[t0 : t0 + 8] = qb * bwd_r[halo + n : halo + n + EDGE].astype(F32)[0:8]

    row0 = lax.broadcasted_iota(jnp.int32, (n, 1), 0) == 0
    h = h_r[...] + jnp.where(row0, gain_r[...], 0.0)
    hsp = dot3(fm, h)
    hr, hi = hsp[0:n], hsp[n:]
    lr = li = None
    for b in range(nb):
        t0 = b * n
        zc, zp = zsp.at[b + 1], zsp.at[b]
        gc, gn = gsp.at[b], gsp.at[b + 1]
        ur = zc[0:n] - zp[n:]
        ui = zc[n:] + zp[0:n]
        gr, gi = gc[0:n], gc[n:]
        dr = gr * ur + gi * ui
        di = gi * ur - gr * ui
        lr = dr if lr is None else lr + dr
        li = di if li is None else li + di
        s = dot3(im, jnp.concatenate([hr * ur - hi * ui, hr * ui + hi * ur], 0))
        gq[t0 : t0 + n] = s * g_r[t0 : t0 + n].astype(F32)
        wr = gr + gn[n:]
        wi = gi - gn[0:n]
        gz = dot3(im, jnp.concatenate([hr * wr + hi * wi, hr * wi - hi * wr], 0))
        gk[t0 : t0 + n] = gz * vf[t0 : t0 + n]
        gv[t0 : t0 + n] = gz * kf[t0 : t0 + n]
    long = dot3(im, jnp.concatenate([lr, li], 0))
    pl_r[...] = long

    hhi = h.astype(BF16)
    hlo = (h - hhi.astype(F32)).astype(BF16)
    hrev = jnp.dot(rev_r[...], jnp.concatenate([hhi, hlo], 0), preferred_element_type=F32)
    g_edge = bwd_r[halo : halo + EDGE].astype(F32)
    for r in range(taps - 1):
        at = length + n - (n - 1) + r
        sr = jnp.sum(hrev * zs[at : at + n], 0, keepdims=True)
        gzr = jnp.sum(h * gs[length + r : length + r + n], 0, keepdims=True)
        gq[length + r : length + r + 1] = sr * g_edge[r : r + 1]
        gk[length + r : length + r + 1] = gzr * vf[length + r : length + r + 1]
        gv[length + r : length + r + 1] = gzr * kf[length + r : length + r + 1]

    rows = []
    for a, (grad, x, base, out) in enumerate(((gq, xq, EDGE, oq_r), (gk, xk, halo, ok_r), (gv, xv, halo, ov_r))):
        sums = [None] * taps
        for b in range(nb):
            t0 = b * n
            own = grad[t0 : t0 + n]
            acc = sf[a][0] * own
            for i in range(1, taps):
                acc = acc + sf[a][i] * grad[t0 + i : t0 + i + n]
            out[t0 : t0 + n] = acc.astype(BF16)
            for i in range(taps):
                part = jnp.sum(own * x[base + t0 - i : base + t0 - i + n], 0, keepdims=True)
                sums[i] = part if sums[i] is None else sums[i] + part
        rows += sums
    rows.append(long[0:1])
    for i, row in enumerate(rows):
        ps_r[i : i + 1] = row


def pack_kernel(halo, length, cw, q_r, k_r, v_r, g_r, *rest):
    outs, sem = rest[:-1], rest[-1]
    copies = []

    def put(src, start, rows, c, dst, at):
        copy = pltpu.make_async_copy(
            src.at[pl.ds(start, rows), pl.ds(c * cw, cw)], dst.at[pl.ds(at, rows)], sem.at[len(copies)]
        )
        copy.start()
        copies.append(copy)

    for c in range(CHUNKS):
        tail, head = outs[2 * c], outs[2 * c + 1]
        put(k_r, length - halo, halo, c, tail, 0)
        put(v_r, length - halo, halo, c, tail, halo)
        put(q_r, length - EDGE, EDGE, c, tail, 2 * halo)
        put(q_r, 0, halo, c, head, 0)
        put(g_r, 0, halo, c, head, halo)
        put(k_r, 0, EDGE, c, head, 2 * halo)
        put(v_r, 0, EDGE, c, head, 2 * halo + EDGE)
    for copy in copies:
        copy.wait()


def shifted(value, axis, by):
    size = lax.axis_size(axis)
    pairs = [(i, i + by) for i in range(size) if 0 <= i + by < size]
    return lax.ppermute(value, axis, pairs)


def reduce_parts(long, small, axis):
    size = lax.axis_size(axis)
    me = lax.axis_index(axis)
    if size & (size - 1):
        return lax.psum_scatter(long, axis, scatter_dimension=0, tiled=True), lax.psum(small, axis)
    piece = long.shape[0] // size
    width = long.shape[1]
    cur = long.reshape((size, piece, width))
    dist = 1
    while dist < size:
        bit = (me // dist) % 2
        pair = cur.reshape((cur.shape[0] // 2, 2, piece, width))
        keep = jnp.where(bit == 0, pair[:, 0], pair[:, 1])
        send = jnp.where(bit == 0, pair[:, 1], pair[:, 0])
        half = keep.shape[0]
        pack = jnp.concatenate([send.reshape(half * piece, width), small], 0)
        got = lax.ppermute(pack, axis, [(i, i ^ dist) for i in range(size)])
        cur = keep + got[: half * piece].reshape(half, piece, width)
        small = small + got[half * piece :]
        dist *= 2
    return cur[0], small


def body(input_q, input_k, input_v, grad_out, short_filters, long_filter, skip_gain):
    length, width = input_q.shape
    taps = short_filters.shape[1]
    n = long_filter.shape[0]
    halo = n + EDGE
    lanes = LANES
    cw = width // CHUNKS
    steps = cw // lanes
    fm, im = matrices(n)
    fm = jnp.asarray(fm)
    im = jnp.asarray(im)
    flip = np.eye(n, dtype=np.float32)[::-1]
    rev = jnp.asarray(np.concatenate([flip, flip], 1).astype(BF16))
    gain = skip_gain.reshape(1, width)
    arrays = (input_q, input_k, input_v, grad_out)
    outs = ()
    packed = pl.pallas_call(
        functools.partial(pack_kernel, halo, length, cw),
        in_specs=[pl.BlockSpec(memory_space=pl.ANY)] * 4,
        out_specs=[pl.BlockSpec(memory_space=pl.ANY)] * (2 * CHUNKS),
        out_shape=[jax.ShapeDtypeStruct((2 * halo + EDGE * (1 + i % 2), cw), BF16) for i in range(2 * CHUNKS)],
        scratch_shapes=[pltpu.SemaphoreType.DMA((7 * CHUNKS,))],
        name="pack",
    )(*arrays)
    halos = [(shifted(packed[2 * c], "seq", 1), shifted(packed[2 * c + 1], "seq", -1)) for c in range(CHUNKS)]
    small_rows = 3 * taps + 1
    parts = []
    for c in range(CHUNKS):
        col = lambda i, c=c: (0, c * steps + i)
        own = lambda i: (0, i)
        full = pl.BlockSpec((length, lanes), col)
        fixed = lambda a: pl.BlockSpec(a.shape, lambda i: (0, 0))
        fwd, bwd = halos[c]
        res = pl.pallas_call(
            functools.partial(kernel, n, length, len(outs)),
            grid=(steps,),
            in_specs=[full] * 4
            + [
                pl.BlockSpec((fwd.shape[0], lanes), own),
                pl.BlockSpec((bwd.shape[0], lanes), own),
                pl.BlockSpec((3, taps, lanes), lambda i, c=c: (0, 0, c * steps + i)),
                pl.BlockSpec((n, lanes), col),
                pl.BlockSpec((1, lanes), col),
                fixed(fm),
                fixed(im),
                fixed(rev),
            ]
            + [pl.BlockSpec(memory_space=pl.ANY)] * len(outs),
            out_specs=[full] * 3 + [pl.BlockSpec((n, lanes), own), pl.BlockSpec((small_rows, lanes), own)],
            out_shape=[jax.ShapeDtypeStruct((length, width), BF16)] * 3
            + [jax.ShapeDtypeStruct((n, cw), F32), jax.ShapeDtypeStruct((small_rows, cw), F32)],
            scratch_shapes=[
                pltpu.VMEM((EDGE + length + halo, lanes), F32),
                pltpu.VMEM((halo + length + EDGE, lanes), F32),
                pltpu.VMEM((halo + length + EDGE, lanes), F32),
                pltpu.VMEM((length + 8, lanes), F32),
                pltpu.VMEM((length + 8, lanes), F32),
                pltpu.VMEM((n + length + 8, lanes), F32),
                pltpu.VMEM((length + n + 8, lanes), F32),
                pltpu.VMEM((length + 8, lanes), F32),
                pltpu.VMEM((length + 8, lanes), F32),
                pltpu.VMEM((length + 8, lanes), F32),
                pltpu.VMEM((length // n + 1, 2 * n, lanes), F32),
                pltpu.VMEM((length // n + 1, 2 * n, lanes), F32),
            ],
            input_output_aliases={12 + j: j for j in range(len(outs))},
            name=f"hyena_bwd_{c}",
        )(*arrays, fwd, bwd, short_filters, long_filter, gain, fm, im, rev, *outs)
        outs = tuple(res[:3])
        parts.append(reduce_parts(res[3], res[4], "seq"))
    grad_long = jnp.concatenate([p[0] for p in parts], 1)
    small = jnp.concatenate([p[1] for p in parts], 1)
    return outs + (grad_long, small[: 3 * taps].reshape(3, taps, width), small[3 * taps])


def solution(mesh):
    return jax.shard_map(
        body,
        mesh=mesh,
        in_specs=(
            P("seq", "ch"),
            P("seq", "ch"),
            P("seq", "ch"),
            P("seq", "ch"),
            P(None, None, "ch"),
            P(None, "ch"),
            P("ch"),
        ),
        out_specs=(
            P("seq", "ch"),
            P("seq", "ch"),
            P("seq", "ch"),
            P("seq", "ch"),
            P(None, None, "ch"),
            P("ch"),
        ),
        check_vma=False,
    )
```
